32 devices in a mesh: rp: 8 (over y, x, core), re: 4 (over z).
Axes of the slice: x: 2, y: 2, z: 4, core: 2. Of those that a mesh axis runs over, the one named last changes fastest.
Arguments:
- coupling: bfloat16 [128, 4, 2, 6, 4096], P('rp', 're'), may hold values from -1.25 to 1.25
- rp_coords: int32 [3, 128], P(None, 'rp'), may hold values from -8 to 8
- degeneracy: int32 [128], P('rp'), may hold values from 1 to 8
- qpoints: int32 [3, 64], replicated, may hold values from 0 to 15
- eigvec: float32 [64, 2, 6, 6], P('rp'), may hold values from -1.75 to 1.75
Outputs:
- coupling_q: float32 [64, 4, 2, 6, 4096], P('rp', None, None, None, 're')
The draws below stay inside these ranges and needn't reach their ends.
All inputs are finite; a program needn't handle non-finite values.
Results may differ from the reference program's by a relative error of at most 0.0042.
Values may be sent and summed in bfloat16 or wider, within the bound.
A program may use at most 64 MiB of HBM per device.

```python
import math
import jax
import jax.numpy as jnp
from jax import lax

NW = 64
MODES = 6
QGRID = 16
RMAX = 8
RP = 128
RE = 4
Q = 64


def plant(drawn, stream_key, smallest, top_value):
    longest = drawn.shape.index(max(drawn.shape))
    spots = []
    for shift in (0, 1):
        where = [jax.random.randint(jax.random.fold_in(stream_key, axis), (), 0, length) for axis, length in enumerate(drawn.shape)]
        where[longest] = (where[longest] + shift) % drawn.shape[longest]
        spots.append(tuple(where))
    return drawn.at[spots[0]].set(smallest).at[spots[1]].set(top_value)


def shard_levels(own_key, dims, pieces, low, top_value):
    gain = 1.0
    for dim, shards_of in pieces:
        steps = jax.random.uniform(jax.random.fold_in(jax.random.fold_in(own_key, 6), dim), (shards_of,), jnp.float32, low / len(pieces), top_value / len(pieces))
        gain = gain * jnp.repeat(jnp.exp(steps), dims[dim] // shards_of).reshape((-1,) + (1,) * (len(dims) - 1 - dim))
    return gain


def centred(rng, extent, width, bound, shards=(), dtype=jnp.bfloat16):
    result = width * jax.random.normal(rng, extent, jnp.float32)
    if shards:
        result = result * shard_levels(rng, extent, shards, -0.22, 0.18)
    return jnp.clip(result, -bound, bound).astype(dtype)


def setup_inputs(seed: int = 0) -> dict:
    streams_of = jax.random.split(jax.random.key(seed), 6)
    return {
        "coupling": centred(streams_of[0], (RP, RE, 2, MODES, NW * NW), (RP // 5) ** -0.5, 1.25, ((0, 8), (1, 4))),
        "rp_coords": plant(jax.random.randint(streams_of[1], (3, RP), 0 - RMAX, RMAX + 1), jax.random.fold_in(streams_of[1], 1), 0 - RMAX, RMAX).astype(jnp.int32),
        "degeneracy": plant(jax.random.randint(streams_of[2], (RP,), 1, 9), jax.random.fold_in(streams_of[2], 1), 1, 8).astype(jnp.int32),
        "qpoints": plant(jax.random.randint(streams_of[3], (3, Q), 0, QGRID), jax.random.fold_in(streams_of[3], 1), 0, QGRID - 1).astype(jnp.int32),
        "eigvec": centred(streams_of[4], (Q, 2, MODES, MODES), (2 * MODES) ** -0.5, 1.75, ((0, 8),), jnp.float32),
    }


def phases(points, coords, degeneracy):
    turns = jnp.mod(points[0][:, None] * coords[0][None, :], QGRID)
    turns = turns + jnp.mod(points[1][:, None] * coords[1][None, :], QGRID)
    turns = turns + jnp.mod(points[2][:, None] * coords[2][None, :], QGRID)
    turns = jnp.mod(turns, QGRID)
    angles = turns.astype(jnp.float32) * (2.0 * math.pi / QGRID)
    weights = 1.0 / degeneracy.astype(jnp.float32)
    table = jnp.concatenate([jnp.cos(angles) * weights[None, :], jnp.sin(angles) * weights[None, :]], axis=0)
    return table.astype(jnp.bfloat16)


def combine(table, coupling):
    point_count = table.shape[0] // 2
    product = jnp.dot(table, coupling.reshape(coupling.shape[0], -1), preferred_element_type=jnp.float32)
    product = product.reshape((2, point_count) + coupling.shape[1:])
    real_part = product[0, :, :, 0] - product[1, :, :, 1]
    imag_part = product[0, :, :, 1] + product[1, :, :, 0]
    return jnp.stack([real_part, imag_part], axis=2)


def mode_mix(values, matrix):
    return jnp.einsum("qrkp,qkn->qrnp", values, matrix, precision=lax.Precision.HIGHEST)


def rotate(summed, eigvec):
    real_in = summed[:, :, 0]
    imag_in = summed[:, :, 1]
    vec_real = eigvec[:, 0]
    vec_imag = eigvec[:, 1]
    real_out = mode_mix(real_in, vec_real) - mode_mix(imag_in, vec_imag)
    imag_out = mode_mix(real_in, vec_imag) + mode_mix(imag_in, vec_real)
    return jnp.stack([real_out, imag_out], axis=2)


def reference(coupling, rp_coords, degeneracy, qpoints, eigvec):
    table = phases(qpoints, rp_coords, degeneracy)
    summed = combine(table, coupling)
    return rotate(summed, eigvec)
```

```python
import functools
import math

import jax
import jax.numpy as jnp
from jax import lax
from jax.experimental import pallas as pl
from jax.experimental.pallas import tpu as pltpu
from jax.sharding import PartitionSpec as P

QGRID = 16
MESH = pl.DeviceIdType.MESH


def phases(points, coords, degeneracy):
    turns = jnp.mod(points[0][:, None] * coords[0][None, :], QGRID)
    turns = turns + jnp.mod(points[1][:, None] * coords[1][None, :], QGRID)
    turns = turns + jnp.mod(points[2][:, None] * coords[2][None, :], QGRID)
    turns = jnp.mod(turns, QGRID)
    angles = turns.astype(jnp.float32) * (2.0 * math.pi / QGRID)
    weights = 1.0 / degeneracy.astype(jnp.float32)
    table = jnp.concatenate(
        [jnp.cos(angles) * weights[None, :], jnp.sin(angles) * weights[None, :]], axis=0
    )
    return table.astype(jnp.bfloat16)


def combine(table, coupling):
    point_count = table.shape[0] // 2
    product = jnp.dot(
        table, coupling.reshape(coupling.shape[0], -1), preferred_element_type=jnp.float32
    )
    product = product.reshape((2, point_count) + coupling.shape[1:])
    real_part = product[0, :, :, 0] - product[1, :, :, 1]
    imag_part = product[0, :, :, 1] + product[1, :, :, 0]
    return jnp.stack([real_part, imag_part], axis=2)


def mode_mix(values, matrix):
    return jnp.einsum("qrkp,qkn->qrnp", values, matrix, precision=lax.Precision.HIGHEST)


def rotate(summed, eigvec):
    real_in = summed[:, :, 0]
    imag_in = summed[:, :, 1]
    vec_real = eigvec[:, 0]
    vec_imag = eigvec[:, 1]
    real_out = mode_mix(real_in, vec_real) - mode_mix(imag_in, vec_imag)
    imag_out = mode_mix(real_in, vec_imag) + mode_mix(imag_in, vec_real)
    return jnp.stack([real_out, imag_out], axis=2)


def to_owners(all_points):
    return lax.all_to_all(all_points, "rp", split_axis=0, concat_axis=3, tiled=True)


def per_device(coupling, rp_coords, degeneracy, qpoints, eigvec):
    stacked = jnp.concatenate([rp_coords, degeneracy[None, :]], axis=0)
    lattice = lax.all_gather(stacked, "rp", axis=1, tiled=True)
    table = phases(qpoints, lattice[:3], lattice[3])
    rp_count = lax.axis_size("rp")
    re_count = lax.axis_size("re")
    local_rp, local_re, parts, mode_count, pair_count = coupling.shape
    q_local = eigvec.shape[0]
    pair_share = pair_count // re_count
    block_cols = mode_count * pair_share
    inner = block_cols // rp_count
    reordered = coupling.reshape(local_rp, local_re, parts, mode_count, re_count, pair_share)
    reordered = jnp.swapaxes(reordered, 3, 4)
    reordered = reordered.reshape(local_rp, local_re, parts, re_count, rp_count, inner)
    reordered = jnp.swapaxes(reordered, 3, 4)
    reordered = reordered.reshape(local_rp, local_re, parts, rp_count * re_count * inner)
    moved = lax.all_to_all(
        lax.all_to_all(reordered, "rp", split_axis=3, concat_axis=0, tiled=True),
        "re",
        split_axis=3,
        concat_axis=1,
        tiled=True,
    )
    all_points = combine(table, moved)
    summed = to_owners(all_points)
    summed = summed.reshape(q_local, summed.shape[1], parts, mode_count, pair_share)
    return rotate(summed, eigvec)


def column_of(angle):
    return [math.cos(2.0 * math.pi * (step - angle) / QGRID) for step in range(QGRID)]


def pick(turns, values):
    picked = jnp.full(turns.shape, values[0], jnp.float32)
    for step in range(1, QGRID):
        picked = jnp.where(turns == step, jnp.float32(values[step]), picked)
    return picked


def far_first(count):
    return sorted(range(count), key=lambda offset: (-min(offset, count - offset), offset))


def exchange_kernel(
    n,
    planes,
    coupling,
    block,
    points,
    out,
    gathered,
    blocks,
    wide,
    columns,
    summed,
    vectors,
    turned,
    outgoing,
    own_sem,
    block_send,
    block_recv,
    first_send,
    first_recv,
    second_send,
    second_recv,
):
    me = lax.axis_index("rp")
    plane = lax.axis_index("re")
    local_rp, _, parts, modes, pairs = coupling.shape
    share = pairs // planes
    lanes = share // n
    q_local = out.shape[0]
    q_count = n * q_local
    total_rp = n * local_rp
    offsets = far_first(planes)

    barrier = pltpu.get_barrier_semaphore()

    def greet(index, carry):
        pl.semaphore_signal(
            barrier,
            inc=1,
            device_id={
                "rp": lax.rem(me + lax.rem(index, n), n),
                "re": lax.rem(plane + index // n, planes),
            },
            device_id_type=MESH,
        )
        return carry

    lax.fori_loop(1, n * planes, greet, 0)
    pl.semaphore_wait(barrier, n * planes - 1)

    def peer(shift):
        return lax.rem(me + shift, n)

    def source(shift):
        return lax.rem(me + n - shift, n)

    def block_copy(shift, slot):
        return pltpu.make_async_remote_copy(
            src_ref=block,
            dst_ref=blocks.at[slot],
            send_sem=block_send.at[shift],
            recv_sem=block_recv.at[slot],
            device_id={"rp": peer(shift)},
            device_id_type=MESH,
        )

    def piece(offset, owner):
        target = lax.rem(plane + offset, planes)
        start = pl.multiple_of(target * share + owner * lanes, lanes)
        return coupling.at[:, 0, :, :, pl.ds(start, lanes)]

    def first_copy(offset, shift, slot):
        return pltpu.make_async_remote_copy(
            src_ref=piece(offset, peer(shift)),
            dst_ref=gathered.at[offset, slot],
            send_sem=first_send.at[offset, shift],
            recv_sem=first_recv.at[offset, slot],
            device_id={"rp": peer(shift)},
            device_id_type=MESH,
        )

    def own_copy(offset):
        return pltpu.make_async_copy(
            piece(offset, me), gathered.at[offset, me], own_sem.at[offset]
        )

    def arrival(offset, slot):
        origin = lax.rem(plane + planes - offset, planes)
        start = pl.multiple_of(slot * lanes, lanes)
        return out.at[:, origin, :, :, pl.ds(start, lanes)]

    def second_copy(offset, shift, slot):
        start = pl.multiple_of(me * lanes, lanes)
        return pltpu.make_async_remote_copy(
            src_ref=outgoing.at[offset, pl.ds(peer(shift) * q_local, q_local)],
            dst_ref=out.at[:, plane, :, :, pl.ds(start, lanes)],
            send_sem=second_send.at[offset, shift],
            recv_sem=second_recv.at[offset, slot],
            device_id={"rp": peer(shift), "re": lax.rem(plane + offset, planes)},
            device_id_type=MESH,
        )

    def second_wait(offset, shift):
        return pltpu.make_async_remote_copy(
            src_ref=outgoing.at[offset, pl.ds(0, q_local)],
            dst_ref=arrival(offset, source(shift)),
            send_sem=second_send.at[offset, shift],
            recv_sem=second_recv.at[offset, source(shift)],
            device_id={"rp": peer(shift), "re": lax.rem(plane + offset, planes)},
            device_id_type=MESH,
        )

    def local_second():
        return pltpu.make_async_copy(
            outgoing.at[0, pl.ds(me * q_local, q_local)],
            arrival(0, me),
            own_sem.at[planes],
        )

    def send_first(offset):
        for shift in range(1, n):
            first_copy(offset, shift, me).start()
        own_copy(offset).start()

    own_block = pltpu.make_async_copy(block, blocks.at[me], own_sem.at[planes + 1])
    own_block.start()
    for shift in range(1, n):
        block_copy(shift, me).start()
    for offset in offsets[:2]:
        send_first(offset)

    own_block.wait()
    for shift in range(1, n):
        block_copy(shift, source(shift)).wait_recv()

    rows = jnp.zeros((8, total_rp), jnp.float32)
    for slot in range(n):
        placed = blocks[slot, q_local:, :]
        rows = rows + (pltpu.roll(placed, slot * local_rp, 1) if slot else placed)
    grid = rows.astype(jnp.int32)
    turns = jnp.zeros((q_count, total_rp), jnp.int32)
    for axis in range(3):
        turns = turns + ((points[:, axis : axis + 1] * grid[axis : axis + 1, :]) & (QGRID - 1))
    turns = turns & (QGRID - 1)
    weights = 1.0 / rows[3:4, :]
    cos = (pick(turns, column_of(0.0)) * weights).astype(jnp.bfloat16)
    sin = (pick(turns, column_of(QGRID / 4)) * weights).astype(jnp.bfloat16)
    table = jnp.concatenate(
        [jnp.concatenate([cos, -sin], axis=1), jnp.concatenate([sin, cos], axis=1)], axis=0
    )

    entries = parts * modes * modes

    def spread(slot, carry):
        held = blocks[slot, :q_local, :]
        rows_at = pl.ds(pl.multiple_of(slot * q_local, q_local), q_local)
        for entry in range(entries):
            vectors[entry, rows_at, :] = jnp.broadcast_to(
                held[:, entry : entry + 1], (q_local, lanes)
            )
        return carry

    lax.fori_loop(0, n, spread, 0)

    for turn, offset in enumerate(offsets):
        own_copy(offset).wait()
        for shift in range(1, n):
            first_copy(offset, shift, source(shift)).wait_recv()

        def widen(slot, carry, offset=offset):
            wide[pl.ds(slot * local_rp, local_rp), :, :modes, :] = gathered[offset, slot].astype(
                jnp.float32
            )
            return carry

        lax.fori_loop(0, n, widen, 0)
        for part in range(parts):
            for mode in range(modes):
                columns[
                    part * total_rp : (part + 1) * total_rp, mode * lanes : (mode + 1) * lanes
                ] = wide[:, part, mode, :].astype(jnp.bfloat16)
        summed[...] = jnp.dot(table, columns[...], preferred_element_type=jnp.float32)

        def rotate_rows(slot, carry):
            start = pl.multiple_of(slot * q_local, q_local)
            rows_at = pl.ds(start, q_local)
            imag_at = pl.ds(q_count + start, q_local)
            real_in = [summed[rows_at, k * lanes : (k + 1) * lanes] for k in range(modes)]
            imag_in = [summed[imag_at, k * lanes : (k + 1) * lanes] for k in range(modes)]
            for mode in range(modes):
                real_out = jnp.zeros((q_local, lanes), jnp.float32)
                imag_out = jnp.zeros((q_local, lanes), jnp.float32)
                for k in range(modes):
                    vec_real = vectors[k * modes + mode, rows_at, :]
                    vec_imag = vectors[(modes + k) * modes + mode, rows_at, :]
                    real_out += real_in[k] * vec_real - imag_in[k] * vec_imag
                    imag_out += real_in[k] * vec_imag + imag_in[k] * vec_real
                turned[rows_at, 0, mode, :] = real_out
                turned[rows_at, 1, mode, :] = imag_out
            return carry

        lax.fori_loop(0, n, rotate_rows, 0)
        outgoing[offset] = turned[:, :, :modes, :].astype(jnp.bfloat16)
        for shift in range(n):
            if offset == 0 and shift == 0:
                local_second().start()
            else:
                second_copy(offset, shift, me).start()
        if turn + 2 < planes:
            send_first(offsets[turn + 2])

    for shift in range(1, n):
        block_copy(shift, me).wait_send()
    for offset in offsets:
        for shift in range(n):
            if shift:
                first_copy(offset, shift, me).wait_send()
            if offset == 0 and shift == 0:
                local_second().wait()
            else:
                second_copy(offset, shift, me).wait_send()
                second_wait(offset, shift).wait_recv()


def exchanged(coupling, rp_coords, degeneracy, qpoints, eigvec):
    n = lax.axis_size("rp")
    planes = lax.axis_size("re")
    local_rp, local_re, parts, modes, pairs = coupling.shape
    q_local = eigvec.shape[0]
    lanes = pairs // planes // n
    total_rp = local_rp * n
    q_count = q_local * n
    entries = parts * modes * modes
    stacked = jnp.concatenate([rp_coords, degeneracy[None, :]], axis=0).astype(jnp.float32)
    block = jnp.concatenate(
        [
            jnp.pad(eigvec.reshape(q_local, entries), ((0, 0), (0, total_rp - entries))),
            jnp.pad(stacked, ((0, 8 - stacked.shape[0]), (0, total_rp - local_rp))),
        ],
        axis=0,
    )
    gathered = pl.pallas_call(
        functools.partial(exchange_kernel, n, planes),
        out_shape=jax.ShapeDtypeStruct((q_local, planes, parts, modes, pairs // planes), jnp.bfloat16),
        in_specs=[
            pl.BlockSpec(memory_space=pl.ANY),
            pl.BlockSpec(memory_space=pl.ANY),
            pl.BlockSpec(memory_space=pltpu.VMEM),
        ],
        out_specs=pl.BlockSpec(memory_space=pl.ANY),
        scratch_shapes=[
            pltpu.VMEM((planes, n, local_rp, parts, modes, lanes), jnp.bfloat16),
            pltpu.VMEM((n, q_local + 8, total_rp), jnp.float32),
            pltpu.VMEM((total_rp, parts, 8, lanes), jnp.float32),
            pltpu.VMEM((parts * total_rp, modes * lanes), jnp.bfloat16),
            pltpu.VMEM((2 * q_count, modes * lanes), jnp.float32),
            pltpu.VMEM((entries, q_count, lanes), jnp.float32),
            pltpu.VMEM((q_count, parts, 8, lanes), jnp.float32),
            pltpu.VMEM((planes, q_count, parts, modes, lanes), jnp.bfloat16),
            pltpu.SemaphoreType.DMA((planes + 2,)),
            pltpu.SemaphoreType.DMA((n,)),
            pltpu.SemaphoreType.DMA((n,)),
            pltpu.SemaphoreType.DMA((planes, n)),
            pltpu.SemaphoreType.DMA((planes, n)),
            pltpu.SemaphoreType.DMA((planes, n)),
            pltpu.SemaphoreType.DMA((planes, n)),
        ],
        compiler_params=pltpu.CompilerParams(collective_id=0, has_side_effects=True),
    )(coupling, block, qpoints.T)
    return gathered.astype(jnp.float32)


def fits(n, planes, coupling, eigvec):
    local_rp, local_re, parts, modes, pairs = coupling.shape
    return (
        local_re == 1
        and parts * modes * modes <= local_rp * n == 128
        and pairs // planes // n == 128
        and eigvec.shape[0] == 8
        and modes <= 8
    )


def either(coupling, rp_coords, degeneracy, qpoints, eigvec):
    if fits(lax.axis_size("rp"), lax.axis_size("re"), coupling, eigvec):
        return exchanged(coupling, rp_coords, degeneracy, qpoints, eigvec)
    return per_device(coupling, rp_coords, degeneracy, qpoints, eigvec)


def solution(mesh):
    return jax.shard_map(
        either,
        mesh=mesh,
        in_specs=(
            P("rp", "re", None, None, None),
            P(None, "rp"),
            P("rp"),
            P(),
            P("rp", None, None, None),
        ),
        out_specs=P("rp", None, None, None, "re"),
        check_vma=False,
    )
```

```python
import functools
import math

import jax
import jax.numpy as jnp
from jax import lax
from jax.experimental import pallas as pl
from jax.experimental.pallas import tpu as pltpu
from jax.sharding import PartitionSpec as P

QGRID = 16
MESH = pl.DeviceIdType.MESH


def phases(points, coords, degeneracy):
    turns = jnp.mod(points[0][:, None] * coords[0][None, :], QGRID)
    turns = turns + jnp.mod(points[1][:, None] * coords[1][None, :], QGRID)
    turns = turns + jnp.mod(points[2][:, None] * coords[2][None, :], QGRID)
    turns = jnp.mod(turns, QGRID)
    angles = turns.astype(jnp.float32) * (2.0 * math.pi / QGRID)
    weights = 1.0 / degeneracy.astype(jnp.float32)
    table = jnp.concatenate(
        [jnp.cos(angles) * weights[None, :], jnp.sin(angles) * weights[None, :]], axis=0
    )
    return table.astype(jnp.bfloat16)


def combine(table, coupling):
    point_count = table.shape[0] // 2
    product = jnp.dot(
        table, coupling.reshape(coupling.shape[0], -1), preferred_element_type=jnp.float32
    )
    product = product.reshape((2, point_count) + coupling.shape[1:])
    real_part = product[0, :, :, 0] - product[1, :, :, 1]
    imag_part = product[0, :, :, 1] + product[1, :, :, 0]
    return jnp.stack([real_part, imag_part], axis=2)


def mode_mix(values, matrix):
    return jnp.einsum("qrkp,qkn->qrnp", values, matrix, precision=lax.Precision.HIGHEST)


def rotate(summed, eigvec):
    real_in = summed[:, :, 0]
    imag_in = summed[:, :, 1]
    vec_real = eigvec[:, 0]
    vec_imag = eigvec[:, 1]
    real_out = mode_mix(real_in, vec_real) - mode_mix(imag_in, vec_imag)
    imag_out = mode_mix(real_in, vec_imag) + mode_mix(imag_in, vec_real)
    return jnp.stack([real_out, imag_out], axis=2)


def to_owners(all_points):
    return lax.all_to_all(all_points, "rp", split_axis=0, concat_axis=3, tiled=True)


def per_device(coupling, rp_coords, degeneracy, qpoints, eigvec):
    stacked = jnp.concatenate([rp_coords, degeneracy[None, :]], axis=0)
    lattice = lax.all_gather(stacked, "rp", axis=1, tiled=True)
    table = phases(qpoints, lattice[:3], lattice[3])
    rp_count = lax.axis_size("rp")
    re_count = lax.axis_size("re")
    local_rp, local_re, parts, mode_count, pair_count = coupling.shape
    q_local = eigvec.shape[0]
    pair_share = pair_count // re_count
    block_cols = mode_count * pair_share
    inner = block_cols // rp_count
    reordered = coupling.reshape(local_rp, local_re, parts, mode_count, re_count, pair_share)
    reordered = jnp.swapaxes(reordered, 3, 4)
    reordered = reordered.reshape(local_rp, local_re, parts, re_count, rp_count, inner)
    reordered = jnp.swapaxes(reordered, 3, 4)
    reordered = reordered.reshape(local_rp, local_re, parts, rp_count * re_count * inner)
    moved = lax.all_to_all(
        lax.all_to_all(reordered, "rp", split_axis=3, concat_axis=0, tiled=True),
        "re",
        split_axis=3,
        concat_axis=1,
        tiled=True,
    )
    all_points = combine(table, moved)
    summed = to_owners(all_points)
    summed = summed.reshape(q_local, summed.shape[1], parts, mode_count, pair_share)
    return rotate(summed, eigvec)


def column_of(angle):
    return [math.cos(2.0 * math.pi * (step - angle) / QGRID) for step in range(QGRID)]


def pick(turns, values):
    picked = jnp.full(turns.shape, values[0], jnp.float32)
    for step in range(1, QGRID):
        picked = jnp.where(turns == step, jnp.float32(values[step]), picked)
    return picked


def far_first(count):
    return sorted(range(count), key=lambda offset: (-min(offset, count - offset), offset))


def exchange_kernel(
    n,
    planes,
    coupling,
    block,
    points,
    out,
    gathered,
    blocks,
    summed,
    vectors,
    turned,
    outgoing,
    own_sem,
    block_send,
    block_recv,
    first_send,
    first_recv,
    second_send,
    second_recv,
):
    me = lax.axis_index("rp")
    plane = lax.axis_index("re")
    local_rp, modes, parts, pairs = coupling.shape
    share = pairs // planes
    lanes = share // n
    q_local = block.shape[0] - 8
    q_count = n * q_local
    q_rows = q_local * modes * parts
    total_rp = n * local_rp
    offsets = far_first(planes)

    barrier = pltpu.get_barrier_semaphore()

    def greet(index, carry):
        pl.semaphore_signal(
            barrier,
            inc=1,
            device_id={
                "rp": lax.rem(me + lax.rem(index, n), n),
                "re": lax.rem(plane + index // n, planes),
            },
            device_id_type=MESH,
        )
        return carry

    lax.fori_loop(1, n * planes, greet, 0)
    pl.semaphore_wait(barrier, n * planes - 1)

    def peer(shift):
        return lax.rem(me + shift, n)

    def source(shift):
        return lax.rem(me + n - shift, n)

    def block_copy(shift, slot):
        return pltpu.make_async_remote_copy(
            src_ref=block,
            dst_ref=blocks.at[slot],
            send_sem=block_send.at[shift],
            recv_sem=block_recv.at[slot],
            device_id={"rp": peer(shift)},
            device_id_type=MESH,
        )

    def piece(offset, owner, mode):
        target = lax.rem(plane + offset, planes)
        start = pl.multiple_of(target * share + owner * lanes, lanes)
        return coupling.at[:, mode, :, pl.ds(start, lanes)]

    def landing(offset, slot, mode):
        return gathered.at[offset, mode, pl.ds(slot * local_rp, local_rp)]

    def first_copy(offset, shift, slot, mode):
        return pltpu.make_async_remote_copy(
            src_ref=piece(offset, peer(shift), mode),
            dst_ref=landing(offset, slot, mode),
            send_sem=first_send.at[offset, shift, mode],
            recv_sem=first_recv.at[offset, slot, mode],
            device_id={"rp": peer(shift)},
            device_id_type=MESH,
        )

    def own_copy(offset, mode):
        return pltpu.make_async_copy(
            piece(offset, me, mode), landing(offset, me, mode), own_sem.at[offset * modes + mode]
        )

    def leaving(offset, owner):
        return outgoing.at[offset, pl.ds(owner * q_local, q_local)]

    def home(origin, slot):
        return out.at[:, origin, :, :, pl.ds(pl.multiple_of(slot * lanes, lanes), lanes)]

    def arrival(offset, slot):
        return home(lax.rem(plane + planes - offset, planes), slot)

    def second_copy(offset, shift, slot):
        return pltpu.make_async_remote_copy(
            src_ref=leaving(offset, peer(shift)),
            dst_ref=home(plane, me),
            send_sem=second_send.at[offset, shift],
            recv_sem=second_recv.at[offset, slot],
            device_id={"rp": peer(shift), "re": lax.rem(plane + offset, planes)},
            device_id_type=MESH,
        )

    def second_wait(offset, shift):
        return pltpu.make_async_remote_copy(
            src_ref=leaving(offset, peer(shift)),
            dst_ref=arrival(offset, source(shift)),
            send_sem=second_send.at[offset, shift],
            recv_sem=second_recv.at[offset, source(shift)],
            device_id={"rp": peer(shift), "re": lax.rem(plane + offset, planes)},
            device_id_type=MESH,
        )

    def local_second():
        return pltpu.make_async_copy(
            leaving(0, me), arrival(0, me), own_sem.at[planes * modes]
        )

    def send_first(offset):
        for mode in range(modes):
            for shift in range(1, n):
                first_copy(offset, shift, me, mode).start()
            own_copy(offset, mode).start()

    own_block = pltpu.make_async_copy(block, blocks.at[me], own_sem.at[planes * modes + 1])
    own_block.start()
    for shift in range(1, n):
        block_copy(shift, me).start()
    for offset in offsets[:2]:
        send_first(offset)

    own_block.wait()
    for shift in range(1, n):
        block_copy(shift, source(shift)).wait_recv()

    rows = jnp.zeros((8, total_rp), jnp.float32)
    for slot in range(n):
        placed = blocks[slot, q_local:, :]
        rows = rows + (pltpu.roll(placed, slot * local_rp, 1) if slot else placed)
    width = parts * total_rp
    repeat = lax.broadcasted_iota(jnp.int32, (total_rp, width), 1) // parts
    repeat = repeat == lax.broadcasted_iota(jnp.int32, (total_rp, width), 0)
    rows = jnp.dot(rows, repeat.astype(jnp.float32), preferred_element_type=jnp.float32)
    grid = rows.astype(jnp.int32)
    turns = jnp.zeros((q_count, width), jnp.int32)
    for axis in range(3):
        turns = turns + ((points[:, axis : axis + 1] * grid[axis : axis + 1, :]) & (QGRID - 1))
    turns = turns & (QGRID - 1)
    weights = 1.0 / rows[3:4, :]
    cos = pick(turns, column_of(0.0)) * weights
    sin = pick(turns, column_of(QGRID / 4)) * weights
    real_part = lax.rem(lax.broadcasted_iota(jnp.int32, (q_count, width), 1), parts) == 0
    table = jnp.concatenate(
        [jnp.where(real_part, cos, -sin), jnp.where(real_part, sin, cos)], axis=0
    ).astype(jnp.bfloat16)

    entries = parts * modes * modes

    def spread(slot, carry):
        held = blocks[slot, :q_local, :]
        rows_at = pl.ds(pl.multiple_of(slot * q_local, q_local), q_local)
        for entry in range(entries):
            vectors[entry, rows_at, :] = jnp.broadcast_to(
                held[:, entry : entry + 1], (q_local, lanes)
            )
        return carry

    lax.fori_loop(0, n, spread, 0)

    for turn, offset in enumerate(offsets):
        for mode in range(modes):
            own_copy(offset, mode).wait()
            for shift in range(1, n):
                first_copy(offset, shift, source(shift), mode).wait_recv()
            summed[:, mode * lanes : (mode + 1) * lanes] = jnp.dot(
                table,
                gathered[offset, mode].reshape(width, lanes),
                preferred_element_type=jnp.float32,
            )

        def rotate_rows(slot, carry):
            start = pl.multiple_of(slot * q_local, q_local)
            rows_at = pl.ds(start, q_local)
            imag_at = pl.ds(q_count + start, q_local)
            real_in = [summed[rows_at, k * lanes : (k + 1) * lanes] for k in range(modes)]
            imag_in = [summed[imag_at, k * lanes : (k + 1) * lanes] for k in range(modes)]
            for mode in range(modes):
                real_out = jnp.zeros((q_local, lanes), jnp.float32)
                imag_out = jnp.zeros((q_local, lanes), jnp.float32)
                for k in range(modes):
                    vec_real = vectors[k * modes + mode, rows_at, :]
                    vec_imag = vectors[(modes + k) * modes + mode, rows_at, :]
                    real_out += real_in[k] * vec_real - imag_in[k] * vec_imag
                    imag_out += real_in[k] * vec_imag + imag_in[k] * vec_real
                first_row = slot * q_rows + mode * parts
                turned[pl.ds(first_row, q_local, stride=modes * parts), :] = real_out
                turned[pl.ds(first_row + 1, q_local, stride=modes * parts), :] = imag_out
            return carry

        lax.fori_loop(0, n, rotate_rows, 0)
        outgoing[offset] = (
            turned[...].astype(jnp.bfloat16).reshape(q_count, modes, parts, lanes)
        )
        for shift in range(n):
            if offset == 0 and shift == 0:
                local_second().start()
            else:
                second_copy(offset, shift, me).start()
        if turn + 2 < planes:
            send_first(offsets[turn + 2])

    for shift in range(1, n):
        block_copy(shift, me).wait_send()
    for offset in offsets:
        for shift in range(n):
            if shift:
                for mode in range(modes):
                    first_copy(offset, shift, me, mode).wait_send()
            if offset == 0 and shift == 0:
                local_second().wait()
            else:
                second_copy(offset, shift, me).wait_send()
                second_wait(offset, shift).wait_recv()


def exchanged(coupling, rp_coords, degeneracy, qpoints, eigvec):
    n = lax.axis_size("rp")
    planes = lax.axis_size("re")
    local_rp, local_re, parts, modes, pairs = coupling.shape
    q_local = eigvec.shape[0]
    lanes = pairs // planes // n
    total_rp = local_rp * n
    q_count = q_local * n
    entries = parts * modes * modes
    stacked = jnp.concatenate([rp_coords, degeneracy[None, :]], axis=0).astype(jnp.float32)
    block = jnp.concatenate(
        [
            jnp.pad(eigvec.reshape(q_local, entries), ((0, 0), (0, total_rp - entries))),
            jnp.pad(stacked, ((0, 8 - stacked.shape[0]), (0, total_rp - local_rp))),
        ],
        axis=0,
    )
    gathered = pl.pallas_call(
        functools.partial(exchange_kernel, n, planes),
        out_shape=jax.ShapeDtypeStruct((q_local, planes, modes, parts, n * lanes), jnp.bfloat16),
        in_specs=[
            pl.BlockSpec(memory_space=pl.ANY),
            pl.BlockSpec(memory_space=pl.ANY),
            pl.BlockSpec(memory_space=pltpu.VMEM),
        ],
        out_specs=pl.BlockSpec(memory_space=pl.ANY),
        scratch_shapes=[
            pltpu.VMEM((planes, modes, total_rp, parts, lanes), jnp.bfloat16),
            pltpu.VMEM((n, q_local + 8, total_rp), jnp.float32),
            pltpu.VMEM((parts * q_count, modes * lanes), jnp.float32),
            pltpu.VMEM((entries, q_count, lanes), jnp.float32),
            pltpu.VMEM((q_count * modes * parts, lanes), jnp.float32),
            pltpu.VMEM((planes, q_count, modes, parts, lanes), jnp.bfloat16),
            pltpu.SemaphoreType.DMA((planes * modes + 2,)),
            pltpu.SemaphoreType.DMA((n,)),
            pltpu.SemaphoreType.DMA((n,)),
            pltpu.SemaphoreType.DMA((planes, n, modes)),
            pltpu.SemaphoreType.DMA((planes, n, modes)),
            pltpu.SemaphoreType.DMA((planes, n)),
            pltpu.SemaphoreType.DMA((planes, n)),
        ],
        compiler_params=pltpu.CompilerParams(collective_id=0, has_side_effects=True),
    )(jnp.swapaxes(coupling[:, 0], 1, 2), block, qpoints.T)
    return jnp.swapaxes(gathered, 2, 3).astype(jnp.float32)


def fits(n, planes, coupling, eigvec):
    local_rp, local_re, parts, modes, pairs = coupling.shape
    return (
        local_re == 1
        and parts * modes * modes <= local_rp * n == 128
        and pairs // planes // n == 128
        and eigvec.shape[0] == 8
        and modes <= 8
    )


def either(coupling, rp_coords, degeneracy, qpoints, eigvec):
    if fits(lax.axis_size("rp"), lax.axis_size("re"), coupling, eigvec):
        return exchanged(coupling, rp_coords, degeneracy, qpoints, eigvec)
    return per_device(coupling, rp_coords, degeneracy, qpoints, eigvec)


def solution(mesh):
    return jax.shard_map(
        either,
        mesh=mesh,
        in_specs=(
            P("rp", "re", None, None, None),
            P(None, "rp"),
            P("rp"),
            P(),
            P("rp", None, None, None),
        ),
        out_specs=P("rp", None, None, None, "re"),
        check_vma=False,
    )
```

```python
import functools
import math

import jax
import jax.numpy as jnp
from jax import lax
from jax.experimental import pallas as pl
from jax.experimental.pallas import tpu as pltpu
from jax.sharding import PartitionSpec as P

QGRID = 16
MESH = pl.DeviceIdType.MESH


def phases(points, coords, degeneracy):
    turns = jnp.mod(points[0][:, None] * coords[0][None, :], QGRID)
    turns = turns + jnp.mod(points[1][:, None] * coords[1][None, :], QGRID)
    turns = turns + jnp.mod(points[2][:, None] * coords[2][None, :], QGRID)
    turns = jnp.mod(turns, QGRID)
    angles = turns.astype(jnp.float32) * (2.0 * math.pi / QGRID)
    weights = 1.0 / degeneracy.astype(jnp.float32)
    table = jnp.concatenate(
        [jnp.cos(angles) * weights[None, :], jnp.sin(angles) * weights[None, :]], axis=0
    )
    return table.astype(jnp.bfloat16)


def combine(table, coupling):
    point_count = table.shape[0] // 2
    product = jnp.dot(
        table, coupling.reshape(coupling.shape[0], -1), preferred_element_type=jnp.float32
    )
    product = product.reshape((2, point_count) + coupling.shape[1:])
    real_part = product[0, :, :, 0] - product[1, :, :, 1]
    imag_part = product[0, :, :, 1] + product[1, :, :, 0]
    return jnp.stack([real_part, imag_part], axis=2)


def mode_mix(values, matrix):
    return jnp.einsum("qrkp,qkn->qrnp", values, matrix, precision=lax.Precision.HIGHEST)


def rotate(summed, eigvec):
    real_in = summed[:, :, 0]
    imag_in = summed[:, :, 1]
    vec_real = eigvec[:, 0]
    vec_imag = eigvec[:, 1]
    real_out = mode_mix(real_in, vec_real) - mode_mix(imag_in, vec_imag)
    imag_out = mode_mix(real_in, vec_imag) + mode_mix(imag_in, vec_real)
    return jnp.stack([real_out, imag_out], axis=2)


def to_owners(all_points):
    return lax.all_to_all(all_points, "rp", split_axis=0, concat_axis=3, tiled=True)


def per_device(coupling, rp_coords, degeneracy, qpoints, eigvec):
    stacked = jnp.concatenate([rp_coords, degeneracy[None, :]], axis=0)
    lattice = lax.all_gather(stacked, "rp", axis=1, tiled=True)
    table = phases(qpoints, lattice[:3], lattice[3])
    rp_count = lax.axis_size("rp")
    re_count = lax.axis_size("re")
    local_rp, local_re, parts, mode_count, pair_count = coupling.shape
    q_local = eigvec.shape[0]
    pair_share = pair_count // re_count
    block_cols = mode_count * pair_share
    inner = block_cols // rp_count
    reordered = coupling.reshape(local_rp, local_re, parts, mode_count, re_count, pair_share)
    reordered = jnp.swapaxes(reordered, 3, 4)
    reordered = reordered.reshape(local_rp, local_re, parts, re_count, rp_count, inner)
    reordered = jnp.swapaxes(reordered, 3, 4)
    reordered = reordered.reshape(local_rp, local_re, parts, rp_count * re_count * inner)
    moved = lax.all_to_all(
        lax.all_to_all(reordered, "rp", split_axis=3, concat_axis=0, tiled=True),
        "re",
        split_axis=3,
        concat_axis=1,
        tiled=True,
    )
    all_points = combine(table, moved)
    summed = to_owners(all_points)
    summed = summed.reshape(q_local, summed.shape[1], parts, mode_count, pair_share)
    return rotate(summed, eigvec)


def column_of(angle):
    return [math.cos(2.0 * math.pi * (step - angle) / QGRID) for step in range(QGRID)]


def pick(turns, values):
    picked = jnp.full(turns.shape, values[0], jnp.float32)
    for step in range(1, QGRID):
        picked = jnp.where(turns == step, jnp.float32(values[step]), picked)
    return picked


def far_first(count):
    return sorted(range(count), key=lambda offset: (-min(offset, count - offset), offset))


def exchange_kernel(
    n,
    planes,
    coupling,
    coords,
    degeneracy,
    eigvec,
    points,
    out,
    gathered,
    all_coords,
    all_degeneracy,
    all_eigvec,
    summed,
    vectors,
    turned,
    outgoing,
    own_sem,
    block_send,
    block_recv,
    first_send,
    first_recv,
    second_send,
    second_recv,
):
    me = lax.axis_index("rp")
    plane = lax.axis_index("re")
    local_rp, modes, parts, pairs = coupling.shape
    share = pairs // planes
    lanes = share // n
    q_local = eigvec.shape[2]
    q_count = n * q_local
    q_rows = q_local * modes * parts
    total_rp = n * local_rp
    offsets = far_first(planes)

    barrier = pltpu.get_barrier_semaphore()

    def greet(index, carry):
        pl.semaphore_signal(
            barrier,
            inc=1,
            device_id={
                "rp": lax.rem(me + lax.rem(index, n), n),
                "re": lax.rem(plane + index // n, planes),
            },
            device_id_type=MESH,
        )
        return carry

    lax.fori_loop(1, n * planes, greet, 0)
    pl.semaphore_wait(barrier, n * planes - 1)

    def peer(shift):
        return lax.rem(me + shift, n)

    def source(shift):
        return lax.rem(me + n - shift, n)

    small = ((coords, all_coords), (degeneracy, all_degeneracy), (eigvec, all_eigvec))

    def block_copies(shift, slot):
        return [
            pltpu.make_async_remote_copy(
                src_ref=held,
                dst_ref=full.at[slot],
                send_sem=block_send.at[shift, index],
                recv_sem=block_recv.at[slot, index],
                device_id={"rp": peer(shift)},
                device_id_type=MESH,
            )
            for index, (held, full) in enumerate(small)
        ]

    def own_blocks():
        return [
            pltpu.make_async_copy(held, full.at[me], own_sem.at[planes * modes + 1 + index])
            for index, (held, full) in enumerate(small)
        ]

    def piece(offset, owner, mode):
        target = lax.rem(plane + offset, planes)
        start = pl.multiple_of(target * share + owner * lanes, lanes)
        return coupling.at[:, mode, :, pl.ds(start, lanes)]

    def landing(offset, slot, mode):
        return gathered.at[offset, mode, pl.ds(slot * local_rp, local_rp)]

    def first_copy(offset, shift, slot, mode):
        return pltpu.make_async_remote_copy(
            src_ref=piece(offset, peer(shift), mode),
            dst_ref=landing(offset, slot, mode),
            send_sem=first_send.at[offset, shift, mode],
            recv_sem=first_recv.at[offset, slot, mode],
            device_id={"rp": peer(shift)},
            device_id_type=MESH,
        )

    def own_copy(offset, mode):
        return pltpu.make_async_copy(
            piece(offset, me, mode), landing(offset, me, mode), own_sem.at[offset * modes + mode]
        )

    def leaving(offset, owner):
        return outgoing.at[offset, pl.ds(owner * q_local, q_local)]

    def home(origin, slot):
        return out.at[:, origin, :, :, pl.ds(pl.multiple_of(slot * lanes, lanes), lanes)]

    def arrival(offset, slot):
        return home(lax.rem(plane + planes - offset, planes), slot)

    def second_copy(offset, shift, slot):
        return pltpu.make_async_remote_copy(
            src_ref=leaving(offset, peer(shift)),
            dst_ref=home(plane, me),
            send_sem=second_send.at[offset, shift],
            recv_sem=second_recv.at[offset, slot],
            device_id={"rp": peer(shift), "re": lax.rem(plane + offset, planes)},
            device_id_type=MESH,
        )

    def second_wait(offset, shift):
        return pltpu.make_async_remote_copy(
            src_ref=leaving(offset, peer(shift)),
            dst_ref=arrival(offset, source(shift)),
            send_sem=second_send.at[offset, shift],
            recv_sem=second_recv.at[offset, source(shift)],
            device_id={"rp": peer(shift), "re": lax.rem(plane + offset, planes)},
            device_id_type=MESH,
        )

    def local_second():
        return pltpu.make_async_copy(
            leaving(0, me), arrival(0, me), own_sem.at[planes * modes]
        )

    def send_first(offset):
        for mode in range(modes):
            for shift in range(1, n):
                first_copy(offset, shift, me, mode).start()
            own_copy(offset, mode).start()

    for shift in range(1, n):
        for copy in block_copies(shift, me):
            copy.start()
    for copy in own_blocks():
        copy.start()
    for offset in offsets[:2]:
        send_first(offset)

    for copy in own_blocks():
        copy.wait()
    for shift in range(1, n):
        for copy in block_copies(shift, source(shift)):
            copy.wait_recv()

    width = parts * total_rp
    repeat = lax.broadcasted_iota(jnp.int32, (total_rp, width), 1) // parts
    repeat = repeat == lax.broadcasted_iota(jnp.int32, (total_rp, width), 0)
    repeat = repeat.astype(jnp.bfloat16)

    def twice(full):
        row = jnp.concatenate([full[slot] for slot in range(n)], axis=1)
        row = row.astype(jnp.float32).astype(jnp.bfloat16)
        return jnp.dot(row, repeat, preferred_element_type=jnp.float32)

    turns = lax.dot_general(
        points[...].astype(jnp.float32).astype(jnp.bfloat16),
        twice(all_coords).astype(jnp.bfloat16),
        (((0,), (0,)), ((), ())),
        preferred_element_type=jnp.float32,
    )
    turns = turns.astype(jnp.int32) & (QGRID - 1)
    weights = 1.0 / twice(all_degeneracy)
    cos = pick(turns, column_of(0.0)) * weights
    sin = pick(turns, column_of(QGRID / 4)) * weights
    real_part = lax.rem(lax.broadcasted_iota(jnp.int32, (q_count, width), 1), parts) == 0
    table = jnp.concatenate(
        [jnp.where(real_part, cos, -sin), jnp.where(real_part, sin, cos)], axis=0
    ).astype(jnp.bfloat16)

    for part in range(parts):
        placed = jnp.concatenate([all_eigvec[slot, :, part, :] for slot in range(n)], axis=1)
        placed = jnp.transpose(placed)
        for entry in range(modes * modes):
            vectors[part * modes * modes + entry] = jnp.broadcast_to(
                placed[:, entry : entry + 1], (q_count, lanes)
            )

    for turn, offset in enumerate(offsets):
        for mode in range(modes):
            own_copy(offset, mode).wait()
            for shift in range(1, n):
                first_copy(offset, shift, source(shift), mode).wait_recv()
            summed[:, mode * lanes : (mode + 1) * lanes] = jnp.dot(
                table,
                gathered[offset, mode].reshape(width, lanes),
                preferred_element_type=jnp.float32,
            )

        def rotate_rows(slot, carry):
            start = pl.multiple_of(slot * q_local, q_local)
            rows_at = pl.ds(start, q_local)
            imag_at = pl.ds(q_count + start, q_local)
            real_in = [summed[rows_at, k * lanes : (k + 1) * lanes] for k in range(modes)]
            imag_in = [summed[imag_at, k * lanes : (k + 1) * lanes] for k in range(modes)]
            for mode in range(modes):
                real_out = jnp.zeros((q_local, lanes), jnp.float32)
                imag_out = jnp.zeros((q_local, lanes), jnp.float32)
                for k in range(modes):
                    vec_real = vectors[k * modes + mode, rows_at, :]
                    vec_imag = vectors[(modes + k) * modes + mode, rows_at, :]
                    real_out += real_in[k] * vec_real - imag_in[k] * vec_imag
                    imag_out += real_in[k] * vec_imag + imag_in[k] * vec_real
                first_row = slot * q_rows + mode * parts
                turned[pl.ds(first_row, q_local, stride=modes * parts), :] = real_out
                turned[pl.ds(first_row + 1, q_local, stride=modes * parts), :] = imag_out
            return carry

        lax.fori_loop(0, n, rotate_rows, 0)
        outgoing[offset] = (
            turned[...].astype(jnp.bfloat16).reshape(q_count, modes, parts, lanes)
        )
        for shift in range(n):
            if offset == 0 and shift == 0:
                local_second().start()
            else:
                second_copy(offset, shift, me).start()
        if turn + 2 < planes:
            send_first(offsets[turn + 2])

    for shift in range(1, n):
        for copy in block_copies(shift, me):
            copy.wait_send()
    for offset in offsets:
        for shift in range(n):
            if shift:
                for mode in range(modes):
                    first_copy(offset, shift, me, mode).wait_send()
            if offset == 0 and shift == 0:
                local_second().wait()
            else:
                second_copy(offset, shift, me).wait_send()
                second_wait(offset, shift).wait_recv()


def exchanged(coupling, rp_coords, degeneracy, qpoints, eigvec):
    n = lax.axis_size("rp")
    planes = lax.axis_size("re")
    local_rp, local_re, parts, modes, pairs = coupling.shape
    q_local = eigvec.shape[0]
    lanes = pairs // planes // n
    total_rp = local_rp * n
    q_count = q_local * n
    entries = parts * modes * modes
    gathered = pl.pallas_call(
        functools.partial(exchange_kernel, n, planes),
        out_shape=jax.ShapeDtypeStruct((q_local, planes, modes, parts, n * lanes), jnp.bfloat16),
        in_specs=[
            pl.BlockSpec(memory_space=pl.ANY),
            pl.BlockSpec(memory_space=pl.ANY),
            pl.BlockSpec(memory_space=pl.ANY),
            pl.BlockSpec(memory_space=pl.ANY),
            pl.BlockSpec(memory_space=pltpu.VMEM),
        ],
        out_specs=pl.BlockSpec(memory_space=pl.ANY),
        scratch_shapes=[
            pltpu.VMEM((planes, modes, total_rp, parts, lanes), jnp.bfloat16),
            pltpu.VMEM((n,) + rp_coords.shape, jnp.int32),
            pltpu.VMEM((n, 1, local_rp), jnp.int32),
            pltpu.VMEM((n, modes * modes, parts, q_local), jnp.float32),
            pltpu.VMEM((parts * q_count, modes * lanes), jnp.float32),
            pltpu.VMEM((entries, q_count, lanes), jnp.float32),
            pltpu.VMEM((q_count * modes * parts, lanes), jnp.float32),
            pltpu.VMEM((planes, q_count, modes, parts, lanes), jnp.bfloat16),
            pltpu.SemaphoreType.DMA((planes * modes + 4,)),
            pltpu.SemaphoreType.DMA((n, 3)),
            pltpu.SemaphoreType.DMA((n, 3)),
            pltpu.SemaphoreType.DMA((planes, n, modes)),
            pltpu.SemaphoreType.DMA((planes, n, modes)),
            pltpu.SemaphoreType.DMA((planes, n)),
            pltpu.SemaphoreType.DMA((planes, n)),
        ],
        compiler_params=pltpu.CompilerParams(collective_id=0, has_side_effects=True),
    )(
        jnp.swapaxes(coupling[:, 0], 1, 2),
        rp_coords,
        degeneracy[None, :],
        jnp.transpose(eigvec, (2, 3, 1, 0)).reshape(modes * modes, parts, q_local),
        qpoints,
    )
    return jnp.swapaxes(gathered, 2, 3).astype(jnp.float32)


def fits(n, planes, coupling, eigvec):
    local_rp, local_re, parts, modes, pairs = coupling.shape
    return (
        local_re == 1
        and parts * modes * modes <= local_rp * n == 128
        and pairs // planes // n == 128
        and eigvec.shape[0] == 8
        and modes <= 8
    )


def either(coupling, rp_coords, degeneracy, qpoints, eigvec):
    if fits(lax.axis_size("rp"), lax.axis_size("re"), coupling, eigvec):
        return exchanged(coupling, rp_coords, degeneracy, qpoints, eigvec)
    return per_device(coupling, rp_coords, degeneracy, qpoints, eigvec)


def solution(mesh):
    return jax.shard_map(
        either,
        mesh=mesh,
        in_specs=(
            P("rp", "re", None, None, None),
            P(None, "rp"),
            P("rp"),
            P(),
            P("rp", None, None, None),
        ),
        out_specs=P("rp", None, None, None, "re"),
        check_vma=False,
    )
```

```python
import functools
import math

import jax
import jax.numpy as jnp
from jax import lax
from jax.experimental import pallas as pl
from jax.experimental.pallas import tpu as pltpu
from jax.sharding import PartitionSpec as P

QGRID = 16
MESH = pl.DeviceIdType.MESH


def phases(points, coords, degeneracy):
    turns = jnp.mod(points[0][:, None] * coords[0][None, :], QGRID)
    turns = turns + jnp.mod(points[1][:, None] * coords[1][None, :], QGRID)
    turns = turns + jnp.mod(points[2][:, None] * coords[2][None, :], QGRID)
    turns = jnp.mod(turns, QGRID)
    angles = turns.astype(jnp.float32) * (2.0 * math.pi / QGRID)
    weights = 1.0 / degeneracy.astype(jnp.float32)
    table = jnp.concatenate(
        [jnp.cos(angles) * weights[None, :], jnp.sin(angles) * weights[None, :]], axis=0
    )
    return table.astype(jnp.bfloat16)


def combine(table, coupling):
    point_count = table.shape[0] // 2
    product = jnp.dot(
        table, coupling.reshape(coupling.shape[0], -1), preferred_element_type=jnp.float32
    )
    product = product.reshape((2, point_count) + coupling.shape[1:])
    real_part = product[0, :, :, 0] - product[1, :, :, 1]
    imag_part = product[0, :, :, 1] + product[1, :, :, 0]
    return jnp.stack([real_part, imag_part], axis=2)


def mode_mix(values, matrix):
    return jnp.einsum("qrkp,qkn->qrnp", values, matrix, precision=lax.Precision.HIGHEST)


def rotate(summed, eigvec):
    real_in = summed[:, :, 0]
    imag_in = summed[:, :, 1]
    vec_real = eigvec[:, 0]
    vec_imag = eigvec[:, 1]
    real_out = mode_mix(real_in, vec_real) - mode_mix(imag_in, vec_imag)
    imag_out = mode_mix(real_in, vec_imag) + mode_mix(imag_in, vec_real)
    return jnp.stack([real_out, imag_out], axis=2)


def to_owners(all_points):
    return lax.all_to_all(all_points, "rp", split_axis=0, concat_axis=3, tiled=True)


def per_device(coupling, rp_coords, degeneracy, qpoints, eigvec):
    stacked = jnp.concatenate([rp_coords, degeneracy[None, :]], axis=0)
    lattice = lax.all_gather(stacked, "rp", axis=1, tiled=True)
    table = phases(qpoints, lattice[:3], lattice[3])
    rp_count = lax.axis_size("rp")
    re_count = lax.axis_size("re")
    local_rp, local_re, parts, mode_count, pair_count = coupling.shape
    q_local = eigvec.shape[0]
    pair_share = pair_count // re_count
    block_cols = mode_count * pair_share
    inner = block_cols // rp_count
    reordered = coupling.reshape(local_rp, local_re, parts, mode_count, re_count, pair_share)
    reordered = jnp.swapaxes(reordered, 3, 4)
    reordered = reordered.reshape(local_rp, local_re, parts, re_count, rp_count, inner)
    reordered = jnp.swapaxes(reordered, 3, 4)
    reordered = reordered.reshape(local_rp, local_re, parts, rp_count * re_count * inner)
    moved = lax.all_to_all(
        lax.all_to_all(reordered, "rp", split_axis=3, concat_axis=0, tiled=True),
        "re",
        split_axis=3,
        concat_axis=1,
        tiled=True,
    )
    all_points = combine(table, moved)
    summed = to_owners(all_points)
    summed = summed.reshape(q_local, summed.shape[1], parts, mode_count, pair_share)
    return rotate(summed, eigvec)


def column_of(angle):
    return [math.cos(2.0 * math.pi * (step - angle) / QGRID) for step in range(QGRID)]


def pick(turns, values):
    picked = jnp.full(turns.shape, values[0], jnp.float32)
    for step in range(1, QGRID):
        picked = jnp.where(turns == step, jnp.float32(values[step]), picked)
    return picked


def far_first(count):
    return sorted(range(count), key=lambda offset: (-min(offset, count - offset), offset))


def exchange_kernel(
    n,
    planes,
    coupling,
    coords,
    degeneracy,
    eigvec,
    points,
    out,
    gathered,
    all_coords,
    all_degeneracy,
    all_eigvec,
    summed,
    vectors,
    turned,
    outgoing,
    own_sem,
    block_send,
    block_recv,
    first_send,
    first_recv,
    second_send,
    second_recv,
):
    me = lax.axis_index("rp")
    plane = lax.axis_index("re")
    local_rp, modes, parts, pairs = coupling.shape
    share = pairs // planes
    lanes = share // n
    q_local = eigvec.shape[0]
    q_count = n * q_local
    q_rows = q_local * modes * parts
    total_rp = n * local_rp
    offsets = far_first(planes)

    barrier = pltpu.get_barrier_semaphore()

    def greet(index, carry):
        pl.semaphore_signal(
            barrier,
            inc=1,
            device_id={
                "rp": lax.rem(me + lax.rem(index, n), n),
                "re": lax.rem(plane + index // n, planes),
            },
            device_id_type=MESH,
        )
        return carry

    lax.fori_loop(1, n * planes, greet, 0)
    pl.semaphore_wait(barrier, n * planes - 1)

    def peer(shift):
        return lax.rem(me + shift, n)

    def source(shift):
        return lax.rem(me + n - shift, n)

    small = ((coords, all_coords), (degeneracy, all_degeneracy), (eigvec, all_eigvec))

    def block_copies(shift, slot):
        return [
            pltpu.make_async_remote_copy(
                src_ref=held,
                dst_ref=full.at[slot],
                send_sem=block_send.at[shift, index],
                recv_sem=block_recv.at[slot, index],
                device_id={"rp": peer(shift)},
                device_id_type=MESH,
            )
            for index, (held, full) in enumerate(small)
        ]

    def own_blocks():
        return [
            pltpu.make_async_copy(held, full.at[me], own_sem.at[planes * modes + 1 + index])
            for index, (held, full) in enumerate(small)
        ]

    def piece(offset, owner, mode):
        target = lax.rem(plane + offset, planes)
        start = pl.multiple_of(target * share + owner * lanes, lanes)
        return coupling.at[:, mode, :, pl.ds(start, lanes)]

    def landing(offset, slot, mode):
        return gathered.at[offset, mode, pl.ds(slot * local_rp, local_rp)]

    def first_copy(offset, shift, slot, mode):
        return pltpu.make_async_remote_copy(
            src_ref=piece(offset, peer(shift), mode),
            dst_ref=landing(offset, slot, mode),
            send_sem=first_send.at[offset, shift, mode],
            recv_sem=first_recv.at[offset, slot, mode],
            device_id={"rp": peer(shift)},
            device_id_type=MESH,
        )

    def own_copy(offset, mode):
        return pltpu.make_async_copy(
            piece(offset, me, mode), landing(offset, me, mode), own_sem.at[offset * modes + mode]
        )

    def leaving(offset, owner):
        return outgoing.at[offset, pl.ds(owner * q_local, q_local)]

    def home(origin, slot):
        return out.at[:, origin, :, :, pl.ds(pl.multiple_of(slot * lanes, lanes), lanes)]

    def arrival(offset, slot):
        return home(lax.rem(plane + planes - offset, planes), slot)

    def second_copy(offset, shift, slot):
        return pltpu.make_async_remote_copy(
            src_ref=leaving(offset, peer(shift)),
            dst_ref=home(plane, me),
            send_sem=second_send.at[offset, shift],
            recv_sem=second_recv.at[offset, slot],
            device_id={"rp": peer(shift), "re": lax.rem(plane + offset, planes)},
            device_id_type=MESH,
        )

    def second_wait(offset, shift):
        return pltpu.make_async_remote_copy(
            src_ref=leaving(offset, peer(shift)),
            dst_ref=arrival(offset, source(shift)),
            send_sem=second_send.at[offset, shift],
            recv_sem=second_recv.at[offset, source(shift)],
            device_id={"rp": peer(shift), "re": lax.rem(plane + offset, planes)},
            device_id_type=MESH,
        )

    def local_second():
        return pltpu.make_async_copy(
            leaving(0, me), arrival(0, me), own_sem.at[planes * modes]
        )

    def send_first(offset):
        for mode in range(modes):
            for shift in range(1, n):
                first_copy(offset, shift, me, mode).start()
            own_copy(offset, mode).start()

    for shift in range(1, n):
        for copy in block_copies(shift, me):
            copy.start()
    for copy in own_blocks():
        copy.start()
    for offset in offsets[:2]:
        send_first(offset)

    for copy in own_blocks():
        copy.wait()
    for shift in range(1, n):
        for copy in block_copies(shift, source(shift)):
            copy.wait_recv()

    width = parts * total_rp
    repeat = lax.broadcasted_iota(jnp.int32, (total_rp, width), 1) // parts
    repeat = repeat == lax.broadcasted_iota(jnp.int32, (total_rp, width), 0)
    repeat = repeat.astype(jnp.bfloat16)

    def twice(full):
        row = jnp.concatenate([full[slot] for slot in range(n)], axis=1)
        row = row.astype(jnp.float32).astype(jnp.bfloat16)
        return jnp.dot(row, repeat, preferred_element_type=jnp.float32)

    turns = lax.dot_general(
        points[...].astype(jnp.float32).astype(jnp.bfloat16),
        twice(all_coords).astype(jnp.bfloat16),
        (((0,), (0,)), ((), ())),
        preferred_element_type=jnp.float32,
    )
    turns = turns.astype(jnp.int32) & (QGRID - 1)
    weights = 1.0 / twice(all_degeneracy)
    cos = pick(turns, column_of(0.0)) * weights
    sin = pick(turns, column_of(QGRID / 4)) * weights
    real_part = lax.rem(lax.broadcasted_iota(jnp.int32, (q_count, width), 1), parts) == 0
    table = jnp.concatenate(
        [jnp.where(real_part, cos, -sin), jnp.where(real_part, sin, cos)], axis=0
    ).astype(jnp.bfloat16)

    placed = all_eigvec[...].reshape(q_count, parts * modes * modes)
    for entry in range(parts * modes * modes):
        vectors[entry] = jnp.broadcast_to(placed[:, entry : entry + 1], (q_count, lanes))

    for turn, offset in enumerate(offsets):
        for mode in range(modes):
            own_copy(offset, mode).wait()
            for shift in range(1, n):
                first_copy(offset, shift, source(shift), mode).wait_recv()
            summed[:, mode * lanes : (mode + 1) * lanes] = jnp.dot(
                table,
                gathered[offset, mode].reshape(width, lanes),
                preferred_element_type=jnp.float32,
            )

        def rotate_rows(slot, carry):
            start = pl.multiple_of(slot * q_local, q_local)
            rows_at = pl.ds(start, q_local)
            imag_at = pl.ds(q_count + start, q_local)
            real_in = [summed[rows_at, k * lanes : (k + 1) * lanes] for k in range(modes)]
            imag_in = [summed[imag_at, k * lanes : (k + 1) * lanes] for k in range(modes)]
            for mode in range(modes):
                real_out = jnp.zeros((q_local, lanes), jnp.float32)
                imag_out = jnp.zeros((q_local, lanes), jnp.float32)
                for k in range(modes):
                    vec_real = vectors[k * modes + mode, rows_at, :]
                    vec_imag = vectors[(modes + k) * modes + mode, rows_at, :]
                    real_out += real_in[k] * vec_real - imag_in[k] * vec_imag
                    imag_out += real_in[k] * vec_imag + imag_in[k] * vec_real
                first_row = slot * q_rows + mode * parts
                turned[pl.ds(first_row, q_local, stride=modes * parts), :] = real_out
                turned[pl.ds(first_row + 1, q_local, stride=modes * parts), :] = imag_out
            return carry

        lax.fori_loop(0, n, rotate_rows, 0)
        outgoing[offset] = (
            turned[...].astype(jnp.bfloat16).reshape(q_count, modes, parts, lanes)
        )
        for shift in range(n):
            if offset == 0 and shift == 0:
                local_second().start()
            else:
                second_copy(offset, shift, me).start()
        if turn + 2 < planes:
            send_first(offsets[turn + 2])

    for shift in range(1, n):
        for copy in block_copies(shift, me):
            copy.wait_send()
    for offset in offsets:
        for shift in range(n):
            if shift:
                for mode in range(modes):
                    first_copy(offset, shift, me, mode).wait_send()
            if offset == 0 and shift == 0:
                local_second().wait()
            else:
                second_copy(offset, shift, me).wait_send()
                second_wait(offset, shift).wait_recv()


def exchanged(coupling, rp_coords, degeneracy, qpoints, eigvec):
    n = lax.axis_size("rp")
    planes = lax.axis_size("re")
    local_rp, local_re, parts, modes, pairs = coupling.shape
    q_local = eigvec.shape[0]
    lanes = pairs // planes // n
    total_rp = local_rp * n
    q_count = q_local * n
    entries = parts * modes * modes
    gathered = pl.pallas_call(
        functools.partial(exchange_kernel, n, planes),
        out_shape=jax.ShapeDtypeStruct((q_local, planes, modes, parts, n * lanes), jnp.bfloat16),
        in_specs=[
            pl.BlockSpec(memory_space=pl.ANY),
            pl.BlockSpec(memory_space=pl.ANY),
            pl.BlockSpec(memory_space=pl.ANY),
            pl.BlockSpec(memory_space=pl.ANY),
            pl.BlockSpec(memory_space=pltpu.VMEM),
        ],
        out_specs=pl.BlockSpec(memory_space=pl.ANY),
        scratch_shapes=[
            pltpu.VMEM((planes, modes, total_rp, parts, lanes), jnp.bfloat16),
            pltpu.VMEM((n,) + rp_coords.shape, jnp.int32),
            pltpu.VMEM((n, 1, local_rp), jnp.int32),
            pltpu.VMEM((n, q_local, entries), jnp.float32),
            pltpu.VMEM((parts * q_count, modes * lanes), jnp.float32),
            pltpu.VMEM((entries, q_count, lanes), jnp.float32),
            pltpu.VMEM((q_count * modes * parts, lanes), jnp.float32),
            pltpu.VMEM((planes, q_count, modes, parts, lanes), jnp.bfloat16),
            pltpu.SemaphoreType.DMA((planes * modes + 4,)),
            pltpu.SemaphoreType.DMA((n, 3)),
            pltpu.SemaphoreType.DMA((n, 3)),
            pltpu.SemaphoreType.DMA((planes, n, modes)),
            pltpu.SemaphoreType.DMA((planes, n, modes)),
            pltpu.SemaphoreType.DMA((planes, n)),
            pltpu.SemaphoreType.DMA((planes, n)),
        ],
        compiler_params=pltpu.CompilerParams(collective_id=0, has_side_effects=True),
    )(
        jnp.swapaxes(coupling[:, 0], 1, 2),
        rp_coords,
        degeneracy[None, :],
        eigvec.reshape(q_local, entries),
        qpoints,
    )
    return jnp.swapaxes(gathered, 2, 3).astype(jnp.float32)


def fits(n, planes, coupling, eigvec):
    local_rp, local_re, parts, modes, pairs = coupling.shape
    return (
        local_re == 1
        and parts * modes * modes <= local_rp * n == 128
        and pairs // planes // n == 128
        and eigvec.shape[0] == 8
        and modes <= 8
    )


def either(coupling, rp_coords, degeneracy, qpoints, eigvec):
    if fits(lax.axis_size("rp"), lax.axis_size("re"), coupling, eigvec):
        return exchanged(coupling, rp_coords, degeneracy, qpoints, eigvec)
    return per_device(coupling, rp_coords, degeneracy, qpoints, eigvec)


def solution(mesh):
    return jax.shard_map(
        either,
        mesh=mesh,
        in_specs=(
            P("rp", "re", None, None, None),
            P(None, "rp"),
            P("rp"),
            P(),
            P("rp", None, None, None),
        ),
        out_specs=P("rp", None, None, None, "re"),
        check_vma=False,
    )
```
